32 devices in a mesh: dp: 8 (over z, core), mp: 4 (over y, x).
Axes of the slice: x: 2, y: 2, z: 4, core: 2. Of those that a mesh axis runs over, the one named last changes fastest.
Arguments:
- inputs: bfloat16 [2048, 4096], P('dp', 'mp'), may hold values from -6 to 6
- out_grads: bfloat16 [2048, 2048], P('dp', 'mp'), may hold values from -6 to 6
- left_old: float32 [4096, 2048], P('dp', 'mp'), may hold values from -2 to 4, as said below
- right_old: float32 [4096, 2048], P('dp', 'mp'), may hold values from -2 to 4, as said below
- left_roots: float32 [4096, 2048], P('dp', 'mp'), may hold values from -2 to 4, as said below
- right_roots: float32 [4096, 2048], P('dp', 'mp'), may hold values from -2 to 4, as said below
- ages: int32 [8, 4], replicated, may hold values from 0 to 199, as said below
Outputs:
- precond: float32 [4096, 2048], P('dp', 'mp')
- left_new: float32 [4096, 2048], P('dp', 'mp')
- right_new: float32 [4096, 2048], P('dp', 'mp')
The draws below stay inside these ranges and needn't reach their ends.
Inputs may be any that keep to these rules, and one draw needn't show every extreme that they name: `ages`: in every row i, blocks (i, j) and (i, j + 2) are never both due, and every row has a due block. `left_old`: every 512 x 512 block is symmetric and positive definite. `right_old`: every 512 x 512 block is symmetric and positive definite. `left_roots`: every 512 x 512 block is symmetric and positive definite. `right_roots`: every 512 x 512 block is symmetric and positive definite.
All inputs are finite; a program needn't handle non-finite values.
Results may differ from the reference program's by a relative error of at most 0.001.
Values may be sent and summed in bfloat16 or wider, within the bound.
No kernel may reach another device: no remote copies, remote signals or barrier semaphores. Data moves between devices by JAX's collectives and lax.ppermute only.
A program may use at most 128 MiB of HBM per device.

```python
import jax
import jax.numpy as jnp
from jax import lax

BS = 512
ITERS = 3
PERIOD = 100
D_IN = 4096
D_OUT = 2048
TOKENS = 2048


def definite_blocks(key, spread, shift):
    rows_blocks = D_IN // BS
    cols_blocks = D_OUT // BS
    base = jax.random.normal(key, (rows_blocks, cols_blocks, BS, BS), jnp.float32)
    gram = jnp.einsum('abij,abkj->abik', base, base) / BS
    stack = spread * gram + shift * jnp.eye(BS, dtype=jnp.float32)
    return stack.transpose(0, 2, 1, 3).reshape(rows_blocks * BS, cols_blocks * BS)


def draw_left_old(key, part):
    return definite_blocks(jax.random.fold_in(key, 11), 1.0, 0.5)


def draw_right_old(key, part):
    return definite_blocks(jax.random.fold_in(key, 12), 1.0, 0.5)


def draw_left_roots(key, part):
    return definite_blocks(jax.random.fold_in(key, 13), 0.5, 0.5)


def draw_right_roots(key, part):
    return definite_blocks(jax.random.fold_in(key, 14), 0.5, 0.5)


def draw_ages(key, part):
    rows_blocks = D_IN // BS
    half_cols = D_OUT // BS // 2
    state = jax.random.randint(jax.random.fold_in(key, 21), (rows_blocks, half_cols), 0, 3)
    forced_col = jax.random.randint(jax.random.fold_in(key, 22), (rows_blocks, 1), 0, half_cols)
    forced_side = jax.random.randint(jax.random.fold_in(key, 23), (rows_blocks, 1), 1, 3)
    column_ids = jnp.arange(half_cols, dtype=jnp.int32)[None, :]
    state = jnp.where(column_ids == forced_col, forced_side, state)
    due_first = jax.random.randint(jax.random.fold_in(key, 24), (rows_blocks, half_cols), PERIOD, 2 * PERIOD)
    due_second = jax.random.randint(jax.random.fold_in(key, 25), (rows_blocks, half_cols), PERIOD, 2 * PERIOD)
    wait_first = jax.random.randint(jax.random.fold_in(key, 26), (rows_blocks, half_cols), 0, PERIOD)
    wait_second = jax.random.randint(jax.random.fold_in(key, 27), (rows_blocks, half_cols), 0, PERIOD)
    first_half = jnp.where(state == 1, due_first, wait_first)
    second_half = jnp.where(state == 2, due_second, wait_second)
    return jnp.concatenate([first_half, second_half], axis=1).astype(jnp.int32)


def levels(stream_key, extent, pieces, least, largest):
    def one(position, blocks):
        draws = jax.random.uniform(jax.random.fold_in(jax.random.fold_in(stream_key, 6), position), (blocks,), jnp.float32, least / len(pieces), largest / len(pieces))
        return jnp.repeat(jnp.exp(draws), extent[position] // blocks).reshape((-1,) + (1,) * (len(extent) - position - 1))

    factor_of = one(*pieces[0])
    for cut in pieces[1:]:
        factor_of = factor_of * one(*cut)
    return factor_of


def scatter_about(own_key, dims, deviation, bound, pieces=(), kind=jnp.bfloat16):
    drawn = deviation * jax.random.normal(own_key, dims, jnp.float32)
    if pieces:
        drawn = drawn * levels(own_key, dims, pieces, -0.22, 0.18)
    return jnp.clip(drawn, -bound, bound).astype(kind)


def setup_inputs(seed: int = 0) -> dict:
    seeds = jax.random.split(jax.random.key(seed), 8)
    inputs = scatter_about(seeds[0], (TOKENS, D_IN), 1.0, 6.0, ((0, 8), (1, 4)))
    out_grads = scatter_about(seeds[1], (TOKENS, D_OUT), 1.0, 6.0, ((0, 8), (1, 4)))
    left_old = draw_left_old(jax.random.fold_in(seeds[7], 71), 0)
    right_old = draw_right_old(jax.random.fold_in(seeds[7], 71), 0)
    left_roots = draw_left_roots(jax.random.fold_in(seeds[7], 71), 0)
    right_roots = draw_right_roots(jax.random.fold_in(seeds[7], 71), 0)
    ages = draw_ages(jax.random.fold_in(seeds[7], 71), 0)
    return {"inputs": inputs, "out_grads": out_grads, "left_old": left_old, "right_old": right_old, "left_roots": left_roots, "right_roots": right_roots, "ages": ages}


decay_rate = 0.95
ridge = 0.001

def product(first, second):
    return jnp.dot(first, second, precision=lax.Precision.HIGHEST, preferred_element_type=jnp.float32)

def gram_rows(matrix):
    return lax.dot_general(matrix, matrix, (((1,), (1,)), ((), ())), precision=lax.Precision.HIGHEST, preferred_element_type=jnp.float32)

def gram_cols(matrix):
    return lax.dot_general(matrix, matrix, (((0,), (0,)), ((), ())), precision=lax.Precision.HIGHEST, preferred_element_type=jnp.float32)

def inverse_root(stat):
    block_order = stat.shape[0]
    identity = jnp.eye(block_order, dtype=jnp.float32)
    matrix = stat + ridge * identity
    norm_scale = jnp.sqrt(jnp.sum(matrix * matrix) / block_order + 1e-06)
    moment = matrix / norm_scale
    inverse = identity
    for iteration in range(ITERS):
        factor = (5.0 * identity - moment) / 4.0
        if iteration == 0:
            inverse = factor * norm_scale ** (-0.25)
        else:
            inverse = product(inverse, factor)
        if iteration + 1 < ITERS:
            square = product(factor, factor)
            moment = product(product(square, square), moment)
    return inverse

def reference(inputs, out_grads, left_old, right_old, left_roots, right_roots, ages):
    gradient = lax.dot_general(inputs.astype(jnp.float32), out_grads.astype(jnp.float32), (((0,), (0,)), ((), ())), precision=lax.Precision.HIGHEST, preferred_element_type=jnp.float32) * TOKENS ** (-0.5)
    rows_blocks = D_IN // BS
    cols_blocks = D_OUT // BS

    def to_blocks(whole):
        return whole.reshape(rows_blocks, BS, cols_blocks, BS).transpose(0, 2, 1, 3).reshape(rows_blocks * cols_blocks, BS, BS)

    def from_blocks(stack):
        return stack.reshape(rows_blocks, cols_blocks, BS, BS).transpose(0, 2, 1, 3).reshape(D_IN, D_OUT)
    refresh = (ages >= PERIOD).reshape(-1)

    def per_block(items):
        block_grad, left_prev, right_prev, left_inv_old, right_inv_old, refresh_due = items
        left_stat = decay_rate * left_prev + gram_rows(block_grad) / BS
        right_stat = decay_rate * right_prev + gram_cols(block_grad) / BS
        left_inv = lax.cond(refresh_due, lambda: inverse_root(left_stat), lambda: left_inv_old)
        right_inv = lax.cond(refresh_due, lambda: inverse_root(right_stat), lambda: right_inv_old)
        return (product(product(left_inv, block_grad), right_inv), left_stat, right_stat)
    precond, left_new, right_new = lax.map(per_block, (to_blocks(gradient), to_blocks(left_old), to_blocks(right_old), to_blocks(left_roots), to_blocks(right_roots), refresh))
    return (from_blocks(precond), from_blocks(left_new), from_blocks(right_new))
```

```python
import functools

import jax
import jax.numpy as jnp
from jax import lax
from jax.experimental import pallas as pl
from jax.experimental.pallas import tpu as pltpu
from jax.sharding import PartitionSpec as P

ITERS = 3
PERIOD = 100
decay_rate = 0.95
ridge = 0.001

f32 = jnp.float32
bf16 = jnp.bfloat16
NN = (((1,), (0,)), ((), ()))
NT = (((1,), (1,)), ((), ()))
TN = (((0,), (0,)), ((), ()))


def mul(first, second, dims):
    return lax.dot_general(first, second, dims, preferred_element_type=f32)


def split(value):
    high = value.astype(bf16)
    return high, (value - high.astype(f32)).astype(bf16)


def fused_body(due_ref, slot_ref, *refs, parts, scale, step):
    n_x, n_d = parts
    x_refs, d_refs, refs = refs[:n_x], refs[n_x : n_x + n_d], refs[n_x + n_d :]
    lo_ref, ro_ref, lr_ref, rr_ref, p_ref, ln_ref, rn_ref = refs[:7]
    gh, gl, th, tl, inv, s, sh, sl, xs, ds = refs[7:]
    n = lo_ref.shape[0]
    rows = range(0, n, step)

    def prod(a, b, r, dims=NN):
        (ah, al), (bh, bl) = a, b
        at = pl.ds(r, step)
        return mul(ah[at, :], bh[...], dims) + mul(ah[at, :], bl[...], dims) + mul(al[at, :], bh[...], dims)

    def put(dst, r, v):
        high, low = split(v)
        dst[0][pl.ds(r, step), :] = high
        dst[1][pl.ds(r, step), :] = low

    per = x_refs[0].shape[0] // n_d
    for m in range(n_x):
        xs[pl.ds(m * n_d * per, n_d * per), :] = x_refs[m][...]
        k = slot_ref[m]
        for d in range(n_d):
            ds[pl.ds((m * n_d + d) * per, per), :] = d_refs[d][pl.ds(pl.multiple_of(k * per, per), per), :]
    g = mul(xs[...], ds[...], TN) * scale
    high, low = split(g)
    gh[...] = high
    gl[...] = low
    th[...] = high.T
    tl[...] = low.T
    for r in rows:
        at = pl.ds(r, step)
        ln_ref[at, :] = decay_rate * lo_ref[at, :] + prod((gh, gl), (gh, gl), r, NT) * (1.0 / n)
        rn_ref[at, :] = decay_rate * ro_ref[at, :] + prod((th, tl), (th, tl), r, NT) * (1.0 / n)
    due = due_ref[0]

    @pl.when(due != 0)
    def _():
        eye = {
            r: lax.broadcasted_iota(jnp.int32, (step, n), 0) + r == lax.broadcasted_iota(jnp.int32, (step, n), 1)
            for r in rows
        }
        norms = []
        for w, stat in enumerate((ln_ref, rn_ref)):
            total = jnp.zeros((8, n), f32)
            for r in rows:
                a = stat[pl.ds(r, step), :] + jnp.where(eye[r], ridge, 0.0)
                total = total + jnp.sum((a * a).reshape(step // 8, 8, n), axis=0)
            norm = jnp.sqrt(jnp.sum(total, axis=(0, 1), keepdims=True) / n + 1e-06)
            norms.append(norm)
            coef = -0.25 / norm
            for r in rows:
                a = stat[pl.ds(r, step), :] + jnp.where(eye[r], ridge, 0.0)
                f = jnp.where(eye[r], 1.25, 0.0) + a * coef
                s[w, 0, pl.ds(r, step), :] = f
                put((sh.at[6 * w], sl.at[6 * w]), r, f)

        def each(a, b, fn):
            for w in range(2):
                ref = lambda j, w=w: (sh.at[6 * w + j], sl.at[6 * w + j])
                for r in rows:
                    fn(w, r, prod(ref(a), ref(b), r), pl.ds(r, step), ref)

        def square(w, r, v, at, ref):
            put(ref(1), r, v)
            put(ref(3), r, v - 1.25 * s[w, 0, at, :])

        def pair(w, r, v, at, ref):
            y = 1.25 * s[w, 0, at, :] + v
            s[w, 1, at, :] = y
            put(ref(4), r, y)
            put(ref(5), r, s[w, 0, at, :] - jnp.where(eye[r], 1.25, 0.0))

        def last(w, r, v, at, ref):
            put((inv.at[2 * w], inv.at[2 * w + 1]), r, (1.25 * s[w, 1, at, :] + v) * lax.rsqrt(jnp.sqrt(norms[w])))

        into = lambda j: lambda w, r, v, at, ref: put(ref(j), r, v)
        each(0, 0, square)
        each(1, 1, into(2))
        each(2, 3, pair)
        each(4, 4, into(1))
        each(4, 5, into(3))
        each(1, 1, into(2))
        each(2, 3, last)

    @pl.when(due == 0)
    def _():
        for r in rows:
            put((inv.at[0], inv.at[1]), r, lr_ref[pl.ds(r, step), :])
            put((inv.at[2], inv.at[3]), r, rr_ref[pl.ds(r, step), :])

    for r in rows:
        put((sh.at[0], sl.at[0]), r, prod((inv.at[0], inv.at[1]), (gh, gl), r))
    for r in rows:
        p_ref[pl.ds(r, step), :] = prod((sh.at[0], sl.at[0]), (inv.at[2], inv.at[3]), r)


def fused(due, slots, xs, ds, lo, ro, lr, rr, tokens):
    n = lo.shape[0]
    vmem = pl.BlockSpec(memory_space=pltpu.VMEM)
    smem = pl.BlockSpec(memory_space=pltpu.SMEM)
    out = jax.ShapeDtypeStruct((n, n), f32)
    half = lambda *k: pltpu.VMEM((*k, n, n), bf16)
    flops = 2 * n * n * (tokens + 60 * n)
    return pl.pallas_call(
        functools.partial(fused_body, parts=(len(xs), len(ds)), scale=tokens**-0.5, step=n // 2),
        out_shape=(out, out, out),
        in_specs=[smem, smem] + [vmem] * (len(xs) + len(ds) + 4),
        out_specs=(vmem, vmem, vmem),
        scratch_shapes=[half(), half(), half(), half(), half(4), pltpu.VMEM((2, 2, n, n), f32), half(12), half(12)]
        + [pltpu.VMEM((tokens, n), bf16)] * 2,
        compiler_params=pltpu.CompilerParams(vmem_limit_bytes=60 << 20),
        cost_estimate=pl.CostEstimate(flops=flops, transcendentals=0, bytes_accessed=7 * n * n * 4),
        name="shampoo",
    )(due, slots, *xs, *ds, lo, ro, lr, rr)


def shards(inputs, out_grads, left_old, right_old, left_roots, right_roots, ages):
    n = left_old.shape[0]
    n_dp, n_mp = lax.axis_size("dp"), lax.axis_size("mp")
    tokens = inputs.shape[0] * n_dp
    row, col = lax.axis_index("dp"), lax.axis_index("mp")
    n_z = n_dp // 2
    core, z = row % 2, row // 2
    per = inputs.shape[0] // n_mp
    per_shard = inputs.shape[1] // n

    def send(value, dp_xor, mp_xor):
        pairs = [(p * n_mp + q, (p ^ dp_xor) * n_mp + (q ^ mp_xor)) for p in range(n_dp) for q in range(n_mp)]
        return lax.ppermute(value, ("dp", "mp"), pairs)

    pick = lambda stack, i: lax.dynamic_index_in_dim(stack, i, 0, keepdims=False)

    slices = inputs.reshape(n_mp, per, inputs.shape[1])
    spread = [pick(slices, col)] + [send(pick(slices, col ^ m), 0, m) for m in range(1, n_mp)]
    stack = jnp.stack(spread).reshape(n_mp, per, per_shard, n)

    def block_of(z_to, c_to):
        block = 2 * z_to + c_to
        m, h = col ^ (block // per_shard), block % per_shard
        return lax.dynamic_slice(stack, (m, 0, h, 0), (1, per, 1, n)).reshape(per, n)

    keep = jnp.stack([block_of(z ^ s, core) for s in range(n_z)])
    swap = send(jnp.stack([block_of(z ^ s, 1 - core) for s in range(n_z)]), 1, 0)
    to_row = [jnp.concatenate([keep[s], swap[s]]) for s in range(n_z)]
    rows = jnp.concatenate([to_row[0]] + [send(to_row[s], 2 * s, 0) for s in range(1, n_z)])
    xs = [rows] + [send(rows, 0, m) for m in range(1, n_mp)]

    own = [out_grads] + [send(out_grads, 2 * s, 0) for s in range(1, n_z)]
    other = send(jnp.concatenate(own), 1, 0).reshape(n_z, *out_grads.shape)
    ds = [part for s in range(n_z) for part in (own[s], other[s])]

    due = (ages[row, col] >= PERIOD).astype(jnp.int32).reshape(1)
    slots = (col ^ jnp.arange(n_mp, dtype=jnp.int32)).astype(jnp.int32)
    return fused(due, slots, xs, ds, left_old, right_old, left_roots, right_roots, tokens)


def solution(mesh):
    spec = P("dp", "mp")
    return jax.shard_map(shards, mesh=mesh, in_specs=(spec,) * 6 + (P(),), out_specs=(spec,) * 3, check_vma=False)
```
